32 devices in a mesh: row: 4 (over z), col: 8 (over y, x, core).
Axes of the slice: x: 2, y: 2, z: 4, core: 2. Of those that a mesh axis runs over, the one named last changes fastest.
Arguments:
- diag_blocks: float32 [8, 16, 512, 512], P('row', 'col'), may hold values from -4 to 16, as said below
- horizontal: bfloat16 [8, 16, 512, 512], P('row', 'col'), may hold values from -0.125 to 0.125
- vertical: bfloat16 [8, 16, 512, 512], P('row', 'col'), may hold values from -0.125 to 0.125
Outputs:
- red_factor: float32 [8, 8, 512, 512], P('row', 'col')
- black_schur: float32 [8, 8, 512, 512], P('row', 'col')
- black_links: bfloat16 [8, 8, 4, 512, 512], P('row', 'col')
The draws below stay inside these ranges and needn't reach their ends.
Inputs may be any that keep to these rules, and one draw needn't show every extreme that they name: `diag_blocks`: every block is symmetric and its eigenvalues are at least 1.
All inputs are finite; a program needn't handle non-finite values.
Results may differ from the reference program's by a relative error of at most 0.0054.
Values may be sent and summed in bfloat16 or wider, within the bound.
No kernel may reach another device: no remote copies, remote signals or barrier semaphores. Data moves between devices by JAX's collectives and lax.ppermute only.
A program may use at most 128 MiB of HBM per device.

```python
import math
import jax
import jax.numpy as jnp
from jax import lax

BLOCK = 512
GRID_ROWS = 8
GRID_COLS = 16


def draw_diag_blocks(key, part):
    first_key = jax.random.fold_in(key, 11)
    second_key = jax.random.fold_in(key, 12)
    factor = jax.random.normal(first_key, (GRID_ROWS, GRID_COLS, BLOCK, BLOCK), jnp.float32)
    levels = jnp.exp(jax.random.uniform(second_key, (GRID_ROWS, GRID_COLS, BLOCK), jnp.float32, 0.0, math.log(4.0)))
    strength = 2.0
    gram = jnp.einsum('rcik,rcjk->rcij', factor, factor, precision=lax.Precision.HIGHEST) * (strength / BLOCK)
    return gram + levels[..., None] * jnp.eye(BLOCK, dtype=jnp.float32)


def block_levels(rng, dims, split, smallest, top_value):
    def one(position, parts):
        heights = jax.random.uniform(jax.random.fold_in(jax.random.fold_in(rng, 6), position), (parts,), jnp.float32, smallest / len(split), top_value / len(split))
        return jnp.repeat(jnp.exp(heights), dims[position] // parts).reshape((-1,) + (1,) * (len(dims) - position - 1))

    level = one(*split[0])
    for cut in split[1:]:
        level = level * one(*cut)
    return level


def gaussian(rng, shape, width, most, pieces=(), kind=jnp.bfloat16):
    factor_of = block_levels(rng, shape, pieces, -0.22, 0.18) if pieces else 1.0
    drawn = jax.random.normal(rng, shape, jnp.float32) * width * factor_of
    return jnp.minimum(jnp.maximum(drawn, -most), most).astype(kind)


def setup_inputs(seed: int = 0) -> dict:
    keys = jax.random.split(jax.random.key(seed), 4)
    diag_blocks = draw_diag_blocks(jax.random.fold_in(keys[3], 71), 0)
    horizontal = gaussian(keys[1], (GRID_ROWS, GRID_COLS, BLOCK, BLOCK), (4 * BLOCK) ** -0.5, 0.125, ((0, 4), (1, 8)))
    vertical = gaussian(keys[2], (GRID_ROWS, GRID_COLS, BLOCK, BLOCK), (4 * BLOCK) ** -0.5, 0.125, ((0, 4), (1, 8)))
    return dict(diag_blocks=diag_blocks, horizontal=horizontal, vertical=vertical)


def select_colour(blocks, parity):
    grid_rows = blocks.shape[0]
    grid_columns = blocks.shape[1]
    trailing = blocks.shape[2:]
    paired = blocks.reshape((grid_rows // 2, 2, grid_columns // 2, 2) + trailing)
    joined = jnp.stack([paired[:, 0, :, parity], paired[:, 1, :, 1 - parity]], 1)
    return joined.reshape((grid_rows, grid_columns // 2) + trailing)

def combine_rows(even_rows, odd_rows):
    joined = jnp.stack([even_rows, odd_rows], 1)
    return joined.reshape((2 * even_rows.shape[0],) + even_rows.shape[1:])

def transposed(blocks):
    return jnp.swapaxes(blocks, -1, -2)

def gram_term(former, latter):
    return jnp.einsum('mka,mkb->mab', former.astype(jnp.float32), latter.astype(jnp.float32), precision=lax.Precision.HIGHEST)

def solve_red(packed):
    factor = jnp.linalg.cholesky(packed[0])
    results = [jax.scipy.linalg.solve_triangular(factor, coupling, lower=True) for coupling in packed[1:]]
    return (factor, jnp.stack(results, 1).astype(jnp.bfloat16))

def black_row(packed):
    diag_black, above, below, left_red, right_red = packed
    update = gram_term(above[:, 3], above[:, 3]) + gram_term(below[:, 1], below[:, 1])
    update = update + gram_term(left_red[:, 2], left_red[:, 2]) + gram_term(right_red[:, 0], right_red[:, 0])
    schur_part = diag_black - update
    east_link = -gram_term(right_red[:, 0], right_red[:, 2])
    south_link = -gram_term(below[:, 1], below[:, 3])
    southeast = -(gram_term(right_red[:, 0], right_red[:, 3]) + gram_term(below[:, 1], below[:, 2]))
    southwest = -(gram_term(left_red[:, 2], left_red[:, 3]) + gram_term(below[:, 1], below[:, 0]))
    links = jnp.stack([east_link, south_link, southeast, southwest], 1).astype(jnp.bfloat16)
    return (schur_part, links)

def reference(diag_blocks, horizontal, vertical):
    left_links = jnp.roll(horizontal, 1, axis=1)
    upper_links = jnp.roll(vertical, 1, axis=0)
    couplings = (transposed(select_colour(left_links, 0)).astype(jnp.float32), transposed(select_colour(upper_links, 0)).astype(jnp.float32), select_colour(horizontal, 0).astype(jnp.float32), select_colour(vertical, 0).astype(jnp.float32))
    red_factor, solved = lax.map(solve_red, (select_colour(diag_blocks, 0),) + couplings)
    above = jnp.roll(solved, 1, axis=0)
    below = jnp.roll(solved, -1, axis=0)
    previous = jnp.roll(solved, 1, axis=1)
    following = jnp.roll(solved, -1, axis=1)
    left_red = combine_rows(solved[0::2], previous[1::2])
    right_red = combine_rows(following[0::2], solved[1::2])
    black_schur, black_links = lax.map(black_row, (select_colour(diag_blocks, 1), above, below, left_red, right_red))
    return (red_factor, black_schur, black_links)
```

```python
import jax
import jax.numpy as jnp
from jax import lax
from jax.experimental import pallas as pl
from jax.experimental.pallas import tpu as pltpu
from jax.sharding import PartitionSpec as P

F32 = jnp.float32
BF16 = jnp.bfloat16
LANES = 128
SUB = 8
STEP = 16


def split(value):
    high = value.astype(BF16)
    low = (value - high.astype(F32)).astype(BF16)
    return high, low


def dot3(left, right, left_dim):
    lh, ll = split(left)
    rh, rl = split(right)
    lefts = jnp.concatenate([lh, lh, ll], left_dim)
    rights = jnp.concatenate([rh, rl, rh], 0)
    return lax.dot_general(lefts, rights, (((left_dim,), (0,)), ((), ())), preferred_element_type=F32)


def spread_row(tile, i):
    return jnp.broadcast_to(tile[i : i + 1, :], (SUB, LANES))


def eliminate(rows, first, below):
    tiles = len(rows)
    cols = [
        [jnp.broadcast_to(rows[t][0][:, first + m : first + m + 1], (SUB, LANES)) for t in range(tiles)]
        for m in range(STEP)
    ]
    roots = [None] * STEP
    for i in range(STEP):
        t0, s = divmod(i, SUB)
        pivot = spread_row(cols[i][t0], s)
        inverse = 1.0 / pivot
        roots[i] = pivot
        factor = [None] * tiles
        for t in range(t0, tiles):
            factor[t] = cols[i][t] * inverse
        factor[t0] = jnp.where(below[s], factor[t0], 0.0)
        for m in range(i + 1, STEP):
            top = spread_row(cols[m][t0], s)
            for t in range(t0, tiles):
                cols[m][t] = cols[m][t] - factor[t] * top
        for g in range(len(rows[0])):
            top = spread_row(rows[t0][g], s)
            for t in range(t0, tiles):
                rows[t][g] = rows[t][g] - factor[t] * top
    scales = []
    sub = lax.broadcasted_iota(jnp.int32, (SUB, LANES), 0)
    for t in range(STEP // SUB):
        piv = roots[t * SUB]
        for s in range(1, SUB):
            piv = jnp.where(sub == s, roots[t * SUB + s], piv)
        scales.append(lax.rsqrt(piv))
    return scales


def factor_body(diags, factors, highs, lows, works, exts, tiles):
    size = works[0].shape[0]
    count = size // LANES
    sub = lax.broadcasted_iota(jnp.int32, (SUB, LANES), 0)
    below = [sub > s for s in range(SUB)]
    r = lax.broadcasted_iota(jnp.int32, (LANES, LANES), 0)
    c = lax.broadcasted_iota(jnp.int32, (LANES, LANES), 1)
    eye = jnp.where(r == c, 1.0, 0.0).astype(F32)
    n = len(works)
    for x in range(n):
        works[x][...] = diags[x][...]
        exts[x][...] = jnp.zeros(exts[x].shape, F32)
    for k in range(count):
        lo, hi = k * LANES, (k + 1) * LANES
        for x in range(n):
            tiles[x][:, :LANES] = works[x][lo:hi, lo:hi]
            tiles[x][:, LANES:] = eye
        for p in range(LANES // STEP):
            for x in range(n):
                start = p * STEP
                stop = min(start + 2 * STEP, LANES)
                rows = [
                    [tiles[x][start + SUB * t : start + SUB * (t + 1), g * LANES : (g + 1) * LANES] for g in range(2)]
                    for t in range((stop - start) // SUB)
                ]
                scales = eliminate(rows, start, below)
                for t in range(len(rows)):
                    for g in range(2):
                        v = rows[t][g]
                        if t < STEP // SUB:
                            v = v * scales[t]
                            rows[t][g] = v
                        tiles[x][start + SUB * t : start + SUB * (t + 1), g * LANES : (g + 1) * LANES] = v
                if stop < LANES:
                    done = jnp.concatenate([jnp.concatenate(rows[t], 1) for t in range(STEP // SUB)], 0)
                    update = dot3(done[:, :LANES], done, 0)
                    tiles[x][stop:, :] = tiles[x][stop:, :] - update[stop:, :]
        for x in range(n):
            upper = jnp.where(c >= r, tiles[x][:, :LANES], 0.0)
            inv = jnp.where(c <= r, tiles[x][:, LANES:], 0.0)
            works[x][lo:hi, lo:hi] = upper
            exts[x][lo:hi, lo:hi] = inv
            if k:
                exts[x][lo:hi, :lo] = dot3(inv, exts[x][lo:hi, :lo], 1)
            if hi < size:
                works[x][lo:hi, hi:] = dot3(inv, works[x][lo:hi, hi:], 1)
                panel = works[x][lo:hi, hi:]
                works[x][hi:, hi:] = works[x][hi:, hi:] - dot3(panel, panel, 0)
                exts[x][hi:, :hi] = exts[x][hi:, :hi] - dot3(panel, exts[x][lo:hi, :hi], 0)
    for x in range(n):
        for k in range(count):
            lo, hi = k * LANES, (k + 1) * LANES
            for q in range(count):
                a, b = q * LANES, (q + 1) * LANES
                if q <= k:
                    factors[x][lo:hi, a:b] = works[x][a:b, lo:hi].T
                else:
                    factors[x][lo:hi, a:b] = jnp.zeros((LANES, LANES), F32)
        w = exts[x][...]
        h, l = split(w)
        highs[x][...] = h
        lows[x][...] = l


def factor_kernel(first, second, factor, high, low, w0, w1, e0, e1, t0, t1):
    factor_body(
        [first.at[0, 0], second.at[0, 0]],
        [factor.at[0, 0], factor.at[1, 0]],
        [high.at[0, 0], high.at[1, 0]],
        [low.at[0, 0], low.at[1, 0]],
        [w0, w1], [e0, e1], [t0, t1],
    )


def factorize(diag_blocks):
    rows, columns, size, _ = diag_blocks.shape
    shape = (rows, columns // 2, size, size)
    out_spec = pl.BlockSpec((2, 1, size, size), lambda a, m: (a, m, 0, 0))
    return pl.pallas_call(
        factor_kernel,
        grid=(rows // 2, columns // 2),
        in_specs=[
            pl.BlockSpec((1, 1, size, size), lambda a, m: (2 * a, 2 * m, 0, 0)),
            pl.BlockSpec((1, 1, size, size), lambda a, m: (2 * a + 1, 2 * m + 1, 0, 0)),
        ],
        out_specs=[out_spec, out_spec, out_spec],
        out_shape=[jax.ShapeDtypeStruct(shape, F32), jax.ShapeDtypeStruct(shape, BF16), jax.ShapeDtypeStruct(shape, BF16)],
        scratch_shapes=[pltpu.VMEM((size, size), F32)] * 4 + [pltpu.VMEM((LANES, 2 * LANES), F32)] * 2,
        name="factor",
    )(diag_blocks, diag_blocks)


def passed_along(value, axis, by):
    size = lax.axis_size(axis)
    return lax.ppermute(value, axis, [(i, (i + by) % size) for i in range(size)])


def select_colour(blocks, parity):
    grid_rows = blocks.shape[0]
    grid_columns = blocks.shape[1]
    trailing = blocks.shape[2:]
    paired = blocks.reshape((grid_rows // 2, 2, grid_columns // 2, 2) + trailing)
    joined = jnp.stack([paired[:, 0, :, parity], paired[:, 1, :, 1 - parity]], 1)
    return joined.reshape((grid_rows, grid_columns // 2) + trailing)


def combine_rows(even_rows, odd_rows):
    joined = jnp.stack([even_rows, odd_rows], 1)
    return joined.reshape((2 * even_rows.shape[0],) + even_rows.shape[1:])


def transposed(blocks):
    return jnp.swapaxes(blocks, -1, -2)


def gram_term(former, latter):
    return jnp.einsum("rmka,rmkb->rmab", former, latter, preferred_element_type=jnp.float32)


def apply_inverse(inverse, coupling):
    return jnp.einsum("rmak,rmkb->rmab", inverse, coupling, preferred_element_type=jnp.float32)


def on_device(diag_blocks, horizontal, vertical):
    edge_column = passed_along(horizontal[:, -1:], "col", 1)
    left_links = jnp.concatenate([edge_column, horizontal[:, :-1]], 1)
    edge_row = passed_along(vertical[-1:], "row", 1)
    upper_links = jnp.concatenate([edge_row, vertical[:-1]], 0)
    couplings = (
        transposed(select_colour(left_links, 0)),
        transposed(select_colour(upper_links, 0)),
        select_colour(horizontal, 0),
        select_colour(vertical, 0),
    )
    red_factor, high, low = factorize(diag_blocks)
    results = [apply_inverse(high, coupling) + apply_inverse(low, coupling) for coupling in couplings]
    solved = jnp.stack(results, 2).astype(jnp.bfloat16)
    got_above = passed_along(solved[-1:, :, 3], "row", 1)
    above_down = jnp.concatenate([got_above, solved[:-1, :, 3]], 0)
    got_below = passed_along(solved[:1], "row", -1)
    below_all = jnp.concatenate([solved[1:], got_below], 0)
    got_left = passed_along(solved[1::2, -1:, 2:4], "col", 1)
    left_pair = combine_rows(
        solved[0::2, :, 2:4], jnp.concatenate([got_left, solved[1::2, :-1, 2:4]], 1)
    )
    right_first, right_rest = passed_along((solved[0::2, :1, 0], solved[0::2, :1, 2:4]), "col", -1)
    right_left = combine_rows(
        jnp.concatenate([solved[0::2, 1:, 0], right_first], 1), solved[1::2, :, 0]
    )
    right_pair = combine_rows(
        jnp.concatenate([solved[0::2, 1:, 2:4], right_rest], 1), solved[1::2, :, 2:4]
    )
    below_up = below_all[:, :, 1]
    update = gram_term(above_down, above_down) + gram_term(below_up, below_up)
    update = (
        update
        + gram_term(left_pair[:, :, 0], left_pair[:, :, 0])
        + gram_term(right_left, right_left)
    )
    black_schur = select_colour(diag_blocks, 1) - update
    east_link = -gram_term(right_left, right_pair[:, :, 0])
    south_link = -gram_term(below_up, below_all[:, :, 3])
    southeast = -(
        gram_term(right_left, right_pair[:, :, 1]) + gram_term(below_up, below_all[:, :, 2])
    )
    southwest = -(
        gram_term(left_pair[:, :, 0], left_pair[:, :, 1]) + gram_term(below_up, below_all[:, :, 0])
    )
    black_links = jnp.stack([east_link, south_link, southeast, southwest], 2).astype(jnp.bfloat16)
    return (red_factor, black_schur, black_links)


def solution(mesh):
    in_specs = (
        P("row", "col", None, None),
        P("row", "col", None, None),
        P("row", "col", None, None),
    )
    out_specs = (
        P("row", "col", None, None),
        P("row", "col", None, None),
        P("row", "col", None, None, None),
    )
    return jax.shard_map(
        on_device, mesh=mesh, in_specs=in_specs, out_specs=out_specs, check_vma=False
    )
```
